128 devices in a mesh: rep: 8 (over z, y_lo), fsdp: 16 (over y_hi, x, core).
Axes of the slice: x: 4, y: 4 (y_hi: 2, y_lo: 2; y = y_hi * 2 + y_lo), z: 4, core: 2. Of those that a mesh axis runs over, the one named last changes fastest.
Arguments:
- tokens: bfloat16 [65536, 2048], P(('rep', 'fsdp')), may hold values from -6 to 6
- norm_gain: float32 [2048], replicated, may hold values from 0.5 to 1.5
- outer_params: float32 [2, 2048, 4096], P(None, 'fsdp'), may hold values from -6 to 6
- momentum: float32 [2, 2048, 4096], P(None, 'fsdp'), may hold values from -6 to 6
- deltas: bfloat16 [8, 2, 2048, 4096], P('rep', None, 'fsdp'), may hold values from -6 to 6
Outputs:
- new_params: float32 [2, 2048, 4096], P(None, 'fsdp')
- new_momentum: float32 [2, 2048, 4096], P(None, 'fsdp')
- hidden: bfloat16 [65536, 4096], P(('rep', 'fsdp'))
The draws below stay inside these ranges and needn't reach their ends.
All inputs are finite; a program needn't handle non-finite values.
Results may differ from the reference program's by a relative error of at most 0.01.
Values may be sent and summed in bfloat16 or wider, within the bound.
A program may use at most 192 MiB of HBM per device.

```python
import math
import jax
import jax.numpy as jnp
from jax import lax

D = 2048
FF = 4096
TOKENS = 65536
N_REP = 8


def block_levels(stream_key, shape, split, least, largest):
    def one(position, blocks):
        heights = jax.random.uniform(jax.random.fold_in(jax.random.fold_in(stream_key, 6), position), (blocks,), jnp.float32, least / len(split), largest / len(split))
        return jnp.repeat(jnp.exp(heights), shape[position] // blocks).reshape((-1,) + (1,) * (len(shape) - position - 1))

    loudness = one(*split[0])
    for cut in split[1:]:
        loudness = loudness * one(*cut)
    return loudness


def normal_values(stream_key, dims, deviation, most, pieces=(), held_as=jnp.bfloat16):
    values = jax.random.normal(stream_key, dims, jnp.float32) * deviation
    if len(pieces) > 0:
        values = block_levels(stream_key, dims, pieces, -0.22, 0.18) * values
    return jnp.clip(values, min=-most, max=most).astype(held_as)


def setup_inputs(seed: int = 0) -> dict:
    key_list = jax.random.split(jax.random.key(seed), 6)
    return {
        "tokens": normal_values(key_list[0], (TOKENS, D), 1.0, 6.0, ((0, 128),)),
        "norm_gain": jnp.clip(1.0 + 0.1 * jax.random.normal(key_list[1], (D,), jnp.float32), 0.5, 1.5),
        "outer_params": normal_values(key_list[2], (2, D, FF), 1.0, 6.0, ((1, 16),), jnp.float32),
        "momentum": normal_values(key_list[3], (2, D, FF), 0.5, 6.0, ((1, 16),), jnp.float32),
        "deltas": normal_values(key_list[4], (N_REP, 2, D, FF), 0.5, 6.0, ((0, 8), (2, 16))),
    }


EPS = 1e-05
MU = 0.9
RATE = 0.7

def reference(tokens, norm_gain, outer_params, momentum, deltas):
    total = jnp.zeros(outer_params.shape, jnp.float32)
    for group in range(N_REP):
        total = total + deltas[group].astype(jnp.float32)
    outer_grad = total / N_REP
    new_momentum = MU * momentum + outer_grad
    new_params = outer_params - RATE * (outer_grad + MU * new_momentum)
    weights = new_params.astype(jnp.bfloat16)
    values = tokens.astype(jnp.float32)
    scale_rows = lax.rsqrt(lax.optimization_barrier(jnp.mean(values * values, axis=-1, keepdims=True)) + EPS)
    normed = (values * scale_rows * norm_gain).astype(jnp.bfloat16)
    factor = 1.0 / math.sqrt(D)
    gate = jnp.dot(normed, weights[0], preferred_element_type=jnp.float32) * factor
    up = jnp.dot(normed, weights[1], preferred_element_type=jnp.float32) * factor
    hidden = (jax.nn.silu(gate) * up).astype(jnp.bfloat16)
    return (new_params, new_momentum, hidden)
```

```python
import functools
import math

import jax
import jax.numpy as jnp
from jax import lax
from jax.experimental import pallas as pl
from jax.experimental.pallas import tpu as pltpu
from jax.sharding import PartitionSpec as P

EPS = 1e-05
MU = 0.9
RATE = 0.7
CORES = 2
WIDTH = 128
ZROWS = 16
AROWS = 8
LAST = 10


def advance(params, moment, summed, groups):
    outer_grad = summed * (1.0 / groups)
    moment_next = MU * moment + outer_grad
    params_next = params - RATE * (outer_grad + MU * moment_next)
    return (params_next, moment_next)


def kernel(
    groups, shards,
    tokens, gain, params, moment, deltas,
    new_params, new_moment, hidden,
    full, own, in1, fwd, in2, zsum, yin, tot, p_buf, m_buf, normed, raw, h_buf, w_out, z_out,
    load_sem, pm_sem, raw_sem, pm_out, h_sem,
    rs1_r, rs2_r, yex_r, ag1_r, ag2_r, pw_r, pz_r, zyc_r, zx1_r, zx2_r, zg1_r, zg2_r,
    x1_r, x2_r, yc0_r, yc1_r, yc2_r, yi_r, ayc_r, ax1_r, ax2_r, tok_r, hid_r,
    rs1_s, rs2_s, yex_s, ag1_s, ag2_s, pw_s, pz_s, zyc_s, zx1_s, zx2_s, zg1_s, zg2_s,
    x1_s, x2_s, yc0_s, yc1_s, yc2_s, yi_s, ayc_s, ax1_s, ax2_s, tok_s, hid_s,
):
    chunks = full.shape[0]
    tall = full.shape[6]
    rows = normed.shape[1]
    f32, bf16 = jnp.float32, jnp.bfloat16
    zr, ar = ZROWS, ZROWS + AROWS
    rep = lax.axis_index("rep")
    mine = lax.axis_index("fsdp")
    z, lo = rep // 2, rep % 2
    core = mine % CORES
    other = 1 - core
    chip = mine // CORES
    x, hi = chip % 4, chip // 4
    far = 1 - hi
    zp, zq, zo = z + 1 - 2 * (z % 2), 3 - z, (z + 2) % 4
    zmat, zrow = z // 2, z % 2
    up, down, across = (x + 1) % 4, (x + 3) % 4, (x + 2) % 4
    cut = (hi + lo) % 2

    def at(z_, lo_, hi_, x_, core_):
        return {"rep": z_ * 2 + lo_, "fsdp": (hi_ * 4 + x_) * CORES + core_}

    to_p, to_q = at(zp, lo, hi, x, core), at(zq, lo, hi, x, core)
    to_in, to_cross = at(z, 1 - lo, hi, x, core), at(z, 1 - lo, far, x, core)
    to_up, to_down = at(z, lo, hi, up, core), at(z, lo, hi, down, core)
    to_pair = at(z, lo, hi, x, other)

    def push(src, dst, send, recv, target):
        pltpu.make_async_remote_copy(
            src_ref=src, dst_ref=dst, send_sem=send, recv_sem=recv,
            device_id=target, device_id_type=pl.DeviceIdType.MESH).start()

    def same(ref, send, recv, target):
        push(ref, ref, send, recv, target)

    def drain(ref, sem):
        pltpu.make_async_copy(ref, ref, sem).wait()

    def columns(half, c):
        return pl.ds(pl.multiple_of((half * chunks + c) * WIDTH, WIDTH), WIDTH)

    def delta_load(c, half):
        return pltpu.make_async_copy(deltas.at[:, :, columns(half, c)], own.at[c, :, half], load_sem.at[c])

    def state_loads(c, half):
        return (
            pltpu.make_async_copy(params.at[:, :, columns(half, c)], p_buf.at[c, :, half], pm_sem.at[c, 0]),
            pltpu.make_async_copy(moment.at[:, :, columns(half, c)], m_buf.at[c, :, half], pm_sem.at[c, 1]),
        )

    def state_stores(c, half):
        return (
            pltpu.make_async_copy(p_buf.at[c, :, half], new_params.at[:, :, columns(half, c)], pm_out.at[0]),
            pltpu.make_async_copy(m_buf.at[c, :, half], new_moment.at[:, :, columns(half, c)], pm_out.at[1]),
        )

    @pl.loop(0, chunks)
    def _(c):
        for half in range(2):
            delta_load(c, half).start()

    raw_load = pltpu.make_async_copy(tokens, raw, raw_sem)
    raw_load.start()

    @pl.loop(0, chunks)
    def _(c):
        for half in range(2):
            for copy in state_loads(c, half):
                copy.start()

    barrier = pltpu.get_barrier_semaphore()
    peers = (to_p, to_q, to_in, to_cross, to_up, to_down, to_pair)
    for target in peers:
        pl.semaphore_signal(barrier, inc=1, device_id=target, device_id_type=pl.DeviceIdType.MESH)
    pl.semaphore_wait(barrier, len(peers))

    factor = 1.0 / math.sqrt(normed.shape[2])
    pieces = 8
    piece = rows // pieces

    def live(c):
        return (c >= 0) & (c < chunks)

    @pl.loop(0, chunks + LAST)
    def _(t):
        c9 = t - 9

        @pl.when(live(c9))
        def _(c=c9):
            drain(full.at[c, 0, 0, 0, :, :, ar:tall], yc2_r.at[c])
            same(full.at[c, cut, far, across, :, :, ar:tall], yi_s.at[2], yi_r.at[c], to_in)

        c8 = t - 8

        @pl.when(live(c8))
        def _(c=c8):
            drain(full.at[c, :, 0, 0, :, :, ar:tall], x2_r.at[c])
            same(full.at[c, cut, hi, across, :, :, ar:tall], yc2_s, yc2_r.at[c], to_cross)
            drain(full.at[c, :, :, 0, :, :, zr:ar], ax1_r.at[c, 0])
            same(full.at[c, 0, :, down, :, :, zr:ar], ax2_s.at[0], ax2_r.at[c], to_up)
            drain(full.at[c, :, :, 0, :, :, zr:ar], ax1_r.at[c, 1])
            same(full.at[c, 1, :, up, :, :, zr:ar], ax2_s.at[1], ax2_r.at[c], to_down)
            drain(full.at[c, :, :, :, 0, 0, 0:zr], zg1_r.at[c])
            for pm, pr in ((zmat, zrow), (zp // 2, zp % 2)):
                same(full.at[c, pm, :, :, 0, pr, 0:zr], zg2_s.at[0], zg2_r.at[c], to_q)
            for pm, pr in ((zmat, zrow), (zq // 2, zq % 2)):
                same(full.at[c, pm, :, :, 1, pr, 0:zr], zg2_s.at[1], zg2_r.at[c], to_p)
            drain(full.at[c, :, 0, 0, :, :, ar:tall], yc1_r.at[c])
            same(full.at[c, cut, far, down, :, :, ar:tall], yi_s.at[1], yi_r.at[c], to_in)
            same(full.at[c, cut, far, up, :, :, ar:tall], yi_s.at[1], yi_r.at[c], to_in)

        c7 = t - 7

        @pl.when(live(c7))
        def _(c=c7):
            drain(full.at[c, :, 0, 0, :, :, ar:tall], x1_r.at[c, 0])
            same(full.at[c, 0, hi, down, :, :, ar:tall], x2_s.at[0], x2_r.at[c], to_up)
            same(full.at[c, cut, hi, down, :, :, ar:tall], yc1_s, yc1_r.at[c], to_cross)
            drain(full.at[c, :, 0, 0, :, :, ar:tall], x1_r.at[c, 1])
            same(full.at[c, 1, hi, up, :, :, ar:tall], x2_s.at[1], x2_r.at[c], to_down)
            same(full.at[c, cut, hi, up, :, :, ar:tall], yc1_s, yc1_r.at[c], to_cross)
            drain(full.at[c, 0, :, 0, :, 0, 0:zr], zx2_r.at[c])
            same(full.at[c, zmat, :, :, 0, zrow, 0:zr], zg1_s.at[0], zg1_r.at[c], to_p)
            same(full.at[c, zmat, :, :, 1, zrow, 0:zr], zg1_s.at[1], zg1_r.at[c], to_q)
            drain(full.at[c, :, 0, 0, :, :, zr:ar], ayc_r.at[c])
            same(full.at[c, :, :, x, :, :, zr:ar], ax1_s.at[0], ax1_r.at[c, 0], to_up)
            same(full.at[c, :, :, x, :, :, zr:ar], ax1_s.at[1], ax1_r.at[c, 1], to_down)
            drain(full.at[c, 0, 0, 0, :, :, ar:tall], yc0_r.at[c])
            same(full.at[c, cut, far, x, :, :, ar:tall], yi_s.at[0], yi_r.at[c], to_in)

        c6 = t - 6

        @pl.when(live(c6))
        def _(c=c6):
            drain(w_out.at[c], pw_r.at[c])
            same(full.at[c, :, hi, x, :, :, ar:tall], x1_s.at[0], x1_r.at[c, 0], to_up)
            same(full.at[c, :, hi, x, :, :, ar:tall], x1_s.at[1], x1_r.at[c, 1], to_down)
            same(full.at[c, :, hi, x, :, :, zr:ar], ayc_s, ayc_r.at[c], to_cross)
            same(full.at[c, cut, hi, x, :, :, ar:tall], yc0_s, yc0_r.at[c], to_cross)
            drain(full.at[c, 0, :, 0, :, 0, 0:zr], zx1_r.at[c, 0])
            same(full.at[c, zmat, :, down, 0, zrow, 0:zr], zx2_s.at[0], zx2_r.at[c], to_up)
            drain(full.at[c, 0, :, 0, :, 0, 0:zr], zx1_r.at[c, 1])
            same(full.at[c, zmat, :, up, 1, zrow, 0:zr], zx2_s.at[1], zx2_r.at[c], to_down)

        c5 = t - 5

        @pl.when(live(c5))
        def _(c=c5):
            drain(in1.at[c], ag2_r.at[c])
            for half in range(2):
                is_mine = core == half
                for q in range(4):
                    p_next, m_next = advance(
                        p_buf[c, q, half], m_buf[c, q, half], tot[c, q, half].astype(f32), groups)
                    p_buf[c, q, half] = p_next
                    m_buf[c, q, half] = m_next
                    weights = p_next[zr:tall].astype(bf16)

                    @pl.when(is_mine)
                    def _(q=q, weights=weights):
                        full[c, q // 2, hi, x, core, q % 2, zr:tall, :] = weights

                    @pl.when(jnp.logical_not(is_mine))
                    def _(q=q, weights=weights):
                        w_out[c, q // 2, q % 2] = weights
            push(w_out.at[c], full.at[c, :, hi, x, core, :, zr:tall], pw_s, pw_r.at[c], to_pair)
            for half in range(2):
                for copy in state_stores(c, half):
                    copy.start()
            drain(full.at[c, 0, 0, 0, :, 0, 0:zr], zyc_r.at[c])
            same(full.at[c, zmat, :, x, :, zrow, 0:zr], zx1_s.at[0], zx1_r.at[c, 0], to_up)
            same(full.at[c, zmat, :, x, :, zrow, 0:zr], zx1_s.at[1], zx1_r.at[c, 1], to_down)

        c4 = t - 4

        @pl.when(live(c4))
        def _(c=c4):
            drain(zsum.at[c], ag1_r.at[c])
            for part in (z, zq):
                same(tot.at[c, part, 0], ag2_s.at[0], ag2_r.at[c], to_p)
            for part in (z, zp):
                same(tot.at[c, part, 1], ag2_s.at[1], ag2_r.at[c], to_q)
            drain(z_out.at[c], pz_r.at[c])
            same(full.at[c, zmat, hi, x, :, zrow, 0:zr], zyc_s, zyc_r.at[c], to_cross)

        c3 = t - 3

        @pl.when(live(c3))
        def _(c=c3):
            drain(yin.at[c], yex_r.at[c])
            tot[c, z] = (zsum[c].astype(f32) + yin[c].astype(f32)).astype(bf16)
            same(tot.at[c, z, 0], ag1_s.at[0], ag1_r.at[c], to_q)
            same(tot.at[c, z, 1], ag1_s.at[1], ag1_r.at[c], to_p)
            drain(p_buf.at[c], pm_sem.at[c, 0])
            drain(m_buf.at[c], pm_sem.at[c, 1])

            def early(half):
                p_next, _ = advance(
                    p_buf[c, z, half, 0:zr], m_buf[c, z, half, 0:zr], tot[c, z, half, 0:zr].astype(f32), groups)
                return p_next.astype(bf16)

            full[c, zmat, hi, x, core, zrow, 0:zr, :] = early(core)
            z_out[c] = early(other)
            push(z_out.at[c], full.at[c, zmat, hi, x, core, zrow, 0:zr], pz_s, pz_r.at[c], to_pair)

        c2 = t - 2

        @pl.when(live(c2))
        def _(c=c2):
            drain(in2.at[c], rs2_r.at[c])
            zsum[c] = (own[c, z].astype(f32) + in1[c, 0].astype(f32) + in2[c].astype(f32)).astype(bf16)
            push(zsum.at[c], yin.at[c], yex_s, yex_r.at[c], to_in)

        c1 = t - 1

        @pl.when(live(c1))
        def _(c=c1):
            drain(in1.at[c], rs1_r.at[c])
            fwd[c, 0] = (own[c, zq, 0].astype(f32) + in1[c, 1, 0].astype(f32)).astype(bf16)
            fwd[c, 1] = (own[c, zp, 1].astype(f32) + in1[c, 1, 1].astype(f32)).astype(bf16)
            push(fwd.at[c, 0], in2.at[c, 0], rs2_s.at[0], rs2_r.at[c], to_q)
            push(fwd.at[c, 1], in2.at[c, 1], rs2_s.at[1], rs2_r.at[c], to_p)

        @pl.when(live(t))
        def _(c=t):
            drain(own.at[c], load_sem.at[c])
            push(own.at[c, zp, 0], in1.at[c, 0, 0], rs1_s.at[0], rs1_r.at[c], to_p)
            push(own.at[c, zo, 0], in1.at[c, 1, 0], rs1_s.at[0], rs1_r.at[c], to_p)
            push(own.at[c, zq, 1], in1.at[c, 0, 1], rs1_s.at[1], rs1_r.at[c], to_q)
            push(own.at[c, zo, 1], in1.at[c, 1, 1], rs1_s.at[1], rs1_r.at[c], to_q)

        @pl.when(t == 0)
        def _():
            raw_load.wait()

        @pl.when(t < pieces)
        def _():
            span = pl.ds(pl.multiple_of(t * piece, piece), piece)
            values = raw[span, :].astype(f32)
            scale = lax.rsqrt(jnp.mean(values * values, axis=-1, keepdims=True) + EPS)
            normed[core, span, :] = (values * scale * gain[...]).astype(bf16)
            same(normed.at[core, span, :], tok_s, tok_r, to_pair)

        @pl.when(t == LAST)
        def _():
            drain(normed.at[0], tok_r)

        c10 = t - LAST

        @pl.when(live(c10))
        def _(c=c10):
            drain(full.at[c, :, :, 0, :, :, ar:tall], yi_r.at[c])
            drain(full.at[c, :, :, 0, :, :, zr:ar], ax2_r.at[c])
            drain(full.at[c, :, :, :, :, 0, 0:zr], zg2_r.at[c])
            depth = normed.shape[2]
            both = jnp.concatenate([full[c, 0].reshape(depth, WIDTH), full[c, 1].reshape(depth, WIDTH)], axis=1)

            @pl.loop(0, 2)
            def _(i):
                pair = jnp.dot(normed[i], both, preferred_element_type=f32) * factor
                gate, up_ = pair[:, 0:WIDTH], pair[:, WIDTH:2 * WIDTH]
                h_buf[c, i] = (gate / (1.0 + jnp.exp(-gate)) * up_).astype(bf16)

                @pl.when(i == core)
                def _():
                    pltpu.make_async_copy(h_buf.at[c, i], hidden.at[:, columns(core, c)], h_sem).start()

                @pl.when(i != core)
                def _():
                    push(h_buf.at[c, i], hidden.at[:, columns(core, c)], hid_s, hid_r, to_pair)

    own_half = h_buf.at[:, 0]
    drain(own_half, h_sem)
    drain(own_half, hid_s)
    drain(own_half, hid_r)
    drain(normed.at[0], tok_s)
    drain(p_buf, pm_out.at[0])
    drain(m_buf, pm_out.at[1])
    for i in range(2):
        drain(own.at[:, 0], rs1_s.at[i])
        drain(fwd.at[:, 0], rs2_s.at[i])
        drain(fwd.at[:, 0], ag1_s.at[i])
        drain(own.at[:, 0], ag2_s.at[i])
        drain(full.at[:, 0, :, 0, :, 0, 0:zr], zx1_s.at[i])
        drain(full.at[:, 0, :, 0, 0, 0, 0:zr], zx2_s.at[i])
        drain(full.at[:, 0, :, :, 0, 0, 0:zr], zg1_s.at[i])
        drain(full.at[:, :, :, :, 0, 0, 0:zr], zg2_s.at[i])
        drain(full.at[:, :, 0, 0, :, :, ar:tall], x1_s.at[i])
        drain(full.at[:, 0, 0, 0, :, :, ar:tall], x2_s.at[i])
        drain(full.at[:, :, :, 0, :, :, zr:ar], ax1_s.at[i])
        drain(full.at[:, 0, :, 0, :, :, zr:ar], ax2_s.at[i])
    drain(zsum, yex_s)
    drain(w_out, pw_s)
    drain(z_out, pz_s)
    drain(full.at[:, 0, 0, 0, :, 0, 0:zr], zyc_s)
    drain(full.at[:, 0, 0, 0, :, :, ar:tall], yc0_s)
    drain(full.at[:, :, 0, 0, :, :, ar:tall], yc1_s)
    drain(full.at[:, 0, 0, 0, :, :, ar:tall], yc2_s)
    drain(full.at[:, :, 0, 0, :, :, zr:ar], ayc_s)
    drain(full.at[:, 0, 0, 0, :, :, ar:tall], yi_s.at[0])
    drain(full.at[:, :, 0, 0, :, :, ar:tall], yi_s.at[1])
    drain(full.at[:, 0, 0, 0, :, :, ar:tall], yi_s.at[2])


def solution(mesh):
    groups, shards = mesh.shape["rep"], mesh.shape["fsdp"]

    def body(tokens, norm_gain, outer_params, momentum, deltas):
        rows, model = tokens.shape
        _, height, hid = outer_params.shape
        chunks = hid // (2 * WIDTH)
        tall = height // 2
        bf16, f32 = jnp.bfloat16, jnp.float32
        dma = pltpu.SemaphoreType.DMA
        anywhere = pl.BlockSpec(memory_space=pl.ANY)
        quarters = (4, tall, hid)

        def strip(*lead):
            return pltpu.VMEM((chunks, *lead, tall, WIDTH), bf16)

        each, two = dma((chunks,)), dma((chunks, 2))
        new_params, new_momentum, hidden = pl.pallas_call(
            functools.partial(kernel, groups, shards),
            out_shape=(
                jax.ShapeDtypeStruct(quarters, f32),
                jax.ShapeDtypeStruct(quarters, f32),
                jax.ShapeDtypeStruct((rows, hid), bf16),
            ),
            in_specs=[anywhere, pl.BlockSpec(memory_space=pltpu.VMEM), anywhere, anywhere, anywhere],
            out_specs=(anywhere, anywhere, anywhere),
            scratch_shapes=[
                strip(2, 2, 4, 2, 2),
                strip(4, 2), strip(2, 2), strip(2), strip(2), strip(2), strip(2), strip(4, 2),
                pltpu.VMEM((chunks, 4, 2, tall, WIDTH), f32),
                pltpu.VMEM((chunks, 4, 2, tall, WIDTH), f32),
                pltpu.VMEM((2, rows, model), bf16),
                pltpu.VMEM((rows, model), bf16),
                pltpu.VMEM((chunks, 2, rows, WIDTH), bf16),
                pltpu.VMEM((chunks, 2, 2, tall - ZROWS, WIDTH), bf16),
                pltpu.VMEM((chunks, ZROWS, WIDTH), bf16),
                each, two, dma, dma((2,)), dma,
                each, each, each, each, each, each, each, each, two, each, each, each,
                two, each, each, each, each, each, each, two, each, dma, dma,
                dma((2,)), dma((2,)), dma, dma((2,)), dma((2,)), dma, dma,
                dma, dma((2,)), dma((2,)), dma((2,)), dma((2,)),
                dma((2,)), dma((2,)), dma, dma, dma, dma((3,)), dma, dma((2,)), dma((2,)), dma, dma,
            ],
            compiler_params=pltpu.CompilerParams(
                collective_id=0, has_side_effects=True, vmem_limit_bytes=62 * 1024 * 1024),
            name="round",
        )(
            tokens, norm_gain.reshape(1, model), outer_params.reshape(quarters), momentum.reshape(quarters),
            deltas.reshape(quarters),
        )
        return (new_params.reshape(outer_params.shape), new_momentum.reshape(momentum.shape), hidden)

    in_specs = (
        P(("rep", "fsdp"), None),
        P(),
        P(None, "fsdp", None),
        P(None, "fsdp", None),
        P("rep", None, "fsdp", None),
    )
    out_specs = (P(None, "fsdp", None), P(None, "fsdp", None), P(("rep", "fsdp"), None))
    return jax.shard_map(body, mesh=mesh, in_specs=in_specs, out_specs=out_specs, check_vma=False)
```

```python
import functools
import math

import jax
import jax.numpy as jnp
from jax import lax
from jax.experimental import pallas as pl
from jax.experimental.pallas import tpu as pltpu
from jax.sharding import PartitionSpec as P

EPS = 1e-05
MU = 0.9
RATE = 0.7
CORES = 2
WIDTH = 128
ZROWS = 16
AROWS = 8
LAGS = (0, 2, 4, 6, 8, 10, 12, 14, 16, 18, 20)
LAST = LAGS[10]
VMEM_LIMIT = 48 * 1024 * 1024


def advance(params, moment, summed, groups):
    outer_grad = summed * (1.0 / groups)
    moment_next = MU * moment + outer_grad
    params_next = params - RATE * (outer_grad + MU * moment_next)
    return (params_next, moment_next)


def kernel(
    groups, shards,
    tokens, gain, params, moment, deltas,
    p_buf, m_buf, h_buf,
    full, own, in1, fwd, in2, zsum, yin, tot, normed, raw, h_out, w_out, z_out,
    load_sem, pm_sem, raw_sem,
    rs1_r, rs2_r, yex_r, ag1_r, ag2_r, pw_r, pz_r, zyc_r, zx1_r, zx2_r, zg1_r, zg2_r,
    x1_r, x2_r, yc0_r, yc1_r, yc2_r, yi_r, ayc_r, ax1_r, ax2_r, tok_r, hid_r,
    rs1_s, rs2_s, yex_s, ag1_s, ag2_s, pw_s, pz_s, zyc_s, zx1_s, zx2_s, zg1_s, zg2_s,
    x1_s, x2_s, yc0_s, yc1_s, yc2_s, yi_s, ayc_s, ax1_s, ax2_s, tok_s, hid_s,
):
    chunks = full.shape[0]
    tall = full.shape[6]
    rows = normed.shape[1]
    f32, bf16 = jnp.float32, jnp.bfloat16
    zr, ar = ZROWS, ZROWS + AROWS
    rep = lax.axis_index("rep")
    mine = lax.axis_index("fsdp")
    z, lo = rep // 2, rep % 2
    core = mine % CORES
    other = 1 - core
    chip = mine // CORES
    x, hi = chip % 4, chip // 4
    far = 1 - hi
    zp, zq, zo = z + 1 - 2 * (z % 2), 3 - z, (z + 2) % 4
    zmat, zrow = z // 2, z % 2
    up, down, across = (x + 1) % 4, (x + 3) % 4, (x + 2) % 4
    cut = (hi + lo) % 2

    def at(z_, lo_, hi_, x_, core_):
        return {"rep": z_ * 2 + lo_, "fsdp": (hi_ * 4 + x_) * CORES + core_}

    to_p, to_q = at(zp, lo, hi, x, core), at(zq, lo, hi, x, core)
    to_in, to_cross = at(z, 1 - lo, hi, x, core), at(z, 1 - lo, far, x, core)
    to_up, to_down = at(z, lo, hi, up, core), at(z, lo, hi, down, core)
    to_pair = at(z, lo, hi, x, other)

    def push(src, dst, send, recv, target):
        pltpu.make_async_remote_copy(
            src_ref=src, dst_ref=dst, send_sem=send, recv_sem=recv,
            device_id=target, device_id_type=pl.DeviceIdType.MESH).start()

    def same(ref, send, recv, target):
        push(ref, ref, send, recv, target)

    def drain(ref, sem):
        pltpu.make_async_copy(ref, ref, sem).wait()

    def columns(half, c):
        return pl.ds(pl.multiple_of((half * chunks + c) * WIDTH, WIDTH), WIDTH)

    def delta_load(c, half):
        return pltpu.make_async_copy(deltas.at[:, :, columns(half, c)], own.at[c, :, half], load_sem.at[c])

    def state_loads(c, half):
        return (
            pltpu.make_async_copy(params.at[:, :, columns(half, c)], p_buf.at[c, :, half], pm_sem.at[c, 0]),
            pltpu.make_async_copy(moment.at[:, :, columns(half, c)], m_buf.at[c, :, half], pm_sem.at[c, 1]),
        )

    @pl.loop(0, chunks)
    def _(c):
        for half in range(2):
            delta_load(c, half).start()

    raw_load = pltpu.make_async_copy(tokens, raw, raw_sem)
    raw_load.start()

    @pl.loop(0, chunks)
    def _(c):
        for half in range(2):
            for copy in state_loads(c, half):
                copy.start()

    barrier = pltpu.get_barrier_semaphore()
    peers = (to_p, to_q, to_in, to_cross, to_up, to_down, to_pair)
    for target in peers:
        pl.semaphore_signal(barrier, inc=1, device_id=target, device_id_type=pl.DeviceIdType.MESH)
    pl.semaphore_wait(barrier, len(peers))

    factor = 1.0 / math.sqrt(normed.shape[2])
    pieces = 8
    piece = rows // pieces

    def live(c):
        return (c >= 0) & (c < chunks)

    @pl.loop(0, chunks + LAST)
    def _(t):
        c9 = t - LAGS[9]

        @pl.when(live(c9))
        def _(c=c9):
            drain(full.at[c, 0, 0, 0, :, :, ar:tall], yc2_r.at[c])
            same(full.at[c, cut, far, across, :, :, ar:tall], yi_s.at[2], yi_r.at[c], to_in)

        c8 = t - LAGS[8]

        @pl.when(live(c8))
        def _(c=c8):
            drain(full.at[c, :, 0, 0, :, :, ar:tall], x2_r.at[c])
            same(full.at[c, cut, hi, across, :, :, ar:tall], yc2_s, yc2_r.at[c], to_cross)
            drain(full.at[c, :, :, 0, :, :, zr:ar], ax1_r.at[c, 0])
            same(full.at[c, 0, :, down, :, :, zr:ar], ax2_s.at[0], ax2_r.at[c], to_up)
            drain(full.at[c, :, :, 0, :, :, zr:ar], ax1_r.at[c, 1])
            same(full.at[c, 1, :, up, :, :, zr:ar], ax2_s.at[1], ax2_r.at[c], to_down)
            drain(full.at[c, :, :, :, 0, 0, 0:zr], zg1_r.at[c])
            for pm, pr in ((zmat, zrow), (zp // 2, zp % 2)):
                same(full.at[c, pm, :, :, 0, pr, 0:zr], zg2_s.at[0], zg2_r.at[c], to_q)
            for pm, pr in ((zmat, zrow), (zq // 2, zq % 2)):
                same(full.at[c, pm, :, :, 1, pr, 0:zr], zg2_s.at[1], zg2_r.at[c], to_p)
            drain(full.at[c, :, 0, 0, :, :, ar:tall], yc1_r.at[c])
            same(full.at[c, cut, far, down, :, :, ar:tall], yi_s.at[1], yi_r.at[c], to_in)
            same(full.at[c, cut, far, up, :, :, ar:tall], yi_s.at[1], yi_r.at[c], to_in)

        c7 = t - LAGS[7]

        @pl.when(live(c7))
        def _(c=c7):
            drain(full.at[c, :, 0, 0, :, :, ar:tall], x1_r.at[c, 0])
            same(full.at[c, 0, hi, down, :, :, ar:tall], x2_s.at[0], x2_r.at[c], to_up)
            same(full.at[c, cut, hi, down, :, :, ar:tall], yc1_s, yc1_r.at[c], to_cross)
            drain(full.at[c, :, 0, 0, :, :, ar:tall], x1_r.at[c, 1])
            same(full.at[c, 1, hi, up, :, :, ar:tall], x2_s.at[1], x2_r.at[c], to_down)
            same(full.at[c, cut, hi, up, :, :, ar:tall], yc1_s, yc1_r.at[c], to_cross)
            drain(full.at[c, 0, :, 0, :, 0, 0:zr], zx2_r.at[c])
            same(full.at[c, zmat, :, :, 0, zrow, 0:zr], zg1_s.at[0], zg1_r.at[c], to_p)
            same(full.at[c, zmat, :, :, 1, zrow, 0:zr], zg1_s.at[1], zg1_r.at[c], to_q)
            drain(full.at[c, :, 0, 0, :, :, zr:ar], ayc_r.at[c])
            same(full.at[c, :, :, x, :, :, zr:ar], ax1_s.at[0], ax1_r.at[c, 0], to_up)
            same(full.at[c, :, :, x, :, :, zr:ar], ax1_s.at[1], ax1_r.at[c, 1], to_down)
            drain(full.at[c, 0, 0, 0, :, :, ar:tall], yc0_r.at[c])
            same(full.at[c, cut, far, x, :, :, ar:tall], yi_s.at[0], yi_r.at[c], to_in)

        c6 = t - LAGS[6]

        @pl.when(live(c6))
        def _(c=c6):
            drain(w_out.at[c], pw_r.at[c])
            same(full.at[c, :, hi, x, :, :, ar:tall], x1_s.at[0], x1_r.at[c, 0], to_up)
            same(full.at[c, :, hi, x, :, :, ar:tall], x1_s.at[1], x1_r.at[c, 1], to_down)
            same(full.at[c, :, hi, x, :, :, zr:ar], ayc_s, ayc_r.at[c], to_cross)
            same(full.at[c, cut, hi, x, :, :, ar:tall], yc0_s, yc0_r.at[c], to_cross)
            drain(full.at[c, 0, :, 0, :, 0, 0:zr], zx1_r.at[c, 0])
            same(full.at[c, zmat, :, down, 0, zrow, 0:zr], zx2_s.at[0], zx2_r.at[c], to_up)
            drain(full.at[c, 0, :, 0, :, 0, 0:zr], zx1_r.at[c, 1])
            same(full.at[c, zmat, :, up, 1, zrow, 0:zr], zx2_s.at[1], zx2_r.at[c], to_down)

        c5 = t - LAGS[5]

        @pl.when(live(c5))
        def _(c=c5):
            drain(in1.at[c], ag2_r.at[c])
            for half in range(2):
                is_mine = core == half
                for q in range(4):
                    p_next, m_next = advance(
                        p_buf[c, q, half], m_buf[c, q, half], tot[c, q, half].astype(f32), groups)
                    p_buf[c, q, half] = p_next
                    m_buf[c, q, half] = m_next
                    weights = p_next[zr:tall].astype(bf16)

                    @pl.when(is_mine)
                    def _(q=q, weights=weights):
                        full[c, q // 2, hi, x, core, q % 2, zr:tall, :] = weights

                    @pl.when(jnp.logical_not(is_mine))
                    def _(q=q, weights=weights):
                        w_out[c, q // 2, q % 2] = weights
            push(w_out.at[c], full.at[c, :, hi, x, core, :, zr:tall], pw_s, pw_r.at[c], to_pair)
            drain(full.at[c, 0, 0, 0, :, 0, 0:zr], zyc_r.at[c])
            same(full.at[c, zmat, :, x, :, zrow, 0:zr], zx1_s.at[0], zx1_r.at[c, 0], to_up)
            same(full.at[c, zmat, :, x, :, zrow, 0:zr], zx1_s.at[1], zx1_r.at[c, 1], to_down)

        c4 = t - LAGS[4]

        @pl.when(live(c4))
        def _(c=c4):
            drain(zsum.at[c], ag1_r.at[c])
            for part in (z, zq):
                same(tot.at[c, part, 0], ag2_s.at[0], ag2_r.at[c], to_p)
            for part in (z, zp):
                same(tot.at[c, part, 1], ag2_s.at[1], ag2_r.at[c], to_q)
            drain(z_out.at[c], pz_r.at[c])
            same(full.at[c, zmat, hi, x, :, zrow, 0:zr], zyc_s, zyc_r.at[c], to_cross)

        c3 = t - LAGS[3]

        @pl.when(live(c3))
        def _(c=c3):
            drain(yin.at[c], yex_r.at[c])
            tot[c, z] = (zsum[c].astype(f32) + yin[c].astype(f32)).astype(bf16)
            same(tot.at[c, z, 0], ag1_s.at[0], ag1_r.at[c], to_q)
            same(tot.at[c, z, 1], ag1_s.at[1], ag1_r.at[c], to_p)
            drain(p_buf.at[c], pm_sem.at[c, 0])
            drain(m_buf.at[c], pm_sem.at[c, 1])

            def early(half):
                p_next, _ = advance(
                    p_buf[c, z, half, 0:zr], m_buf[c, z, half, 0:zr], tot[c, z, half, 0:zr].astype(f32), groups)
                return p_next.astype(bf16)

            full[c, zmat, hi, x, core, zrow, 0:zr, :] = early(core)
            z_out[c] = early(other)
            push(z_out.at[c], full.at[c, zmat, hi, x, core, zrow, 0:zr], pz_s, pz_r.at[c], to_pair)

        c2 = t - LAGS[2]

        @pl.when(live(c2))
        def _(c=c2):
            drain(in2.at[c], rs2_r.at[c])
            zsum[c] = (own[c, z].astype(f32) + in1[c, 0].astype(f32) + in2[c].astype(f32)).astype(bf16)
            push(zsum.at[c], yin.at[c], yex_s, yex_r.at[c], to_in)

        c1 = t - LAGS[1]

        @pl.when(live(c1))
        def _(c=c1):
            drain(in1.at[c], rs1_r.at[c])
            fwd[c, 0] = (own[c, zq, 0].astype(f32) + in1[c, 1, 0].astype(f32)).astype(bf16)
            fwd[c, 1] = (own[c, zp, 1].astype(f32) + in1[c, 1, 1].astype(f32)).astype(bf16)
            push(fwd.at[c, 0], in2.at[c, 0], rs2_s.at[0], rs2_r.at[c], to_q)
            push(fwd.at[c, 1], in2.at[c, 1], rs2_s.at[1], rs2_r.at[c], to_p)

        @pl.when(live(t))
        def _(c=t):
            drain(own.at[c], load_sem.at[c])
            push(own.at[c, zp, 0], in1.at[c, 0, 0], rs1_s.at[0], rs1_r.at[c], to_p)
            push(own.at[c, zo, 0], in1.at[c, 1, 0], rs1_s.at[0], rs1_r.at[c], to_p)
            push(own.at[c, zq, 1], in1.at[c, 0, 1], rs1_s.at[1], rs1_r.at[c], to_q)
            push(own.at[c, zo, 1], in1.at[c, 1, 1], rs1_s.at[1], rs1_r.at[c], to_q)

        @pl.when(t == 0)
        def _():
            raw_load.wait()

        @pl.when(t < pieces)
        def _():
            span = pl.ds(pl.multiple_of(t * piece, piece), piece)
            values = raw[span, :].astype(f32)
            scale = lax.rsqrt(jnp.mean(values * values, axis=-1, keepdims=True) + EPS)
            normed[core, span, :] = (values * scale * gain[...]).astype(bf16)
            same(normed.at[core, span, :], tok_s, tok_r, to_pair)

        @pl.when(t == LAST)
        def _():
            drain(normed.at[0], tok_r)

        c10 = t - LAST

        @pl.when(live(c10))
        def _(c=c10):
            drain(full.at[c, :, :, 0, :, :, ar:tall], yi_r.at[c])
            drain(full.at[c, :, :, 0, :, :, zr:ar], ax2_r.at[c])
            drain(full.at[c, :, :, :, :, 0, 0:zr], zg2_r.at[c])
            depth = normed.shape[2]
            both = jnp.concatenate([full[c, 0].reshape(depth, WIDTH), full[c, 1].reshape(depth, WIDTH)], axis=1)

            @pl.loop(0, 2)
            def _(i):
                pair = jnp.dot(normed[i], both, preferred_element_type=f32) * factor
                gate, up_ = pair[:, 0:WIDTH], pair[:, WIDTH:2 * WIDTH]
                out = (gate / (1.0 + jnp.exp(-gate)) * up_).astype(bf16)

                @pl.when(i == core)
                def _():
                    h_buf[core, c] = out

                @pl.when(i != core)
                def _():
                    h_out[c] = out
                    push(h_out.at[c], h_buf.at[core, c], hid_s, hid_r, to_pair)

    drain(h_out, hid_s)
    drain(h_out, hid_r)
    drain(normed.at[0], tok_s)
    for i in range(2):
        drain(own.at[:, 0], rs1_s.at[i])
        drain(fwd.at[:, 0], rs2_s.at[i])
        drain(fwd.at[:, 0], ag1_s.at[i])
        drain(own.at[:, 0], ag2_s.at[i])
        drain(full.at[:, 0, :, 0, :, 0, 0:zr], zx1_s.at[i])
        drain(full.at[:, 0, :, 0, 0, 0, 0:zr], zx2_s.at[i])
        drain(full.at[:, 0, :, :, 0, 0, 0:zr], zg1_s.at[i])
        drain(full.at[:, :, :, :, 0, 0, 0:zr], zg2_s.at[i])
        drain(full.at[:, :, 0, 0, :, :, ar:tall], x1_s.at[i])
        drain(full.at[:, 0, 0, 0, :, :, ar:tall], x2_s.at[i])
        drain(full.at[:, :, :, 0, :, :, zr:ar], ax1_s.at[i])
        drain(full.at[:, 0, :, 0, :, :, zr:ar], ax2_s.at[i])
    drain(zsum, yex_s)
    drain(w_out, pw_s)
    drain(z_out, pz_s)
    drain(full.at[:, 0, 0, 0, :, 0, 0:zr], zyc_s)
    drain(full.at[:, 0, 0, 0, :, :, ar:tall], yc0_s)
    drain(full.at[:, :, 0, 0, :, :, ar:tall], yc1_s)
    drain(full.at[:, 0, 0, 0, :, :, ar:tall], yc2_s)
    drain(full.at[:, :, 0, 0, :, :, zr:ar], ayc_s)
    drain(full.at[:, 0, 0, 0, :, :, ar:tall], yi_s.at[0])
    drain(full.at[:, :, 0, 0, :, :, ar:tall], yi_s.at[1])
    drain(full.at[:, 0, 0, 0, :, :, ar:tall], yi_s.at[2])


def settle(p_buf, m_buf, h_buf, new_params, new_moment, hidden, sems):
    _, chunks, _, _ = h_buf.shape

    def copies(half, c):
        at = pl.ds(pl.multiple_of((half * chunks + c) * WIDTH, WIDTH), WIDTH)
        return (
            pltpu.make_async_copy(p_buf.at[c, :, half], new_params.at[:, :, at], sems.at[0]),
            pltpu.make_async_copy(m_buf.at[c, :, half], new_moment.at[:, :, at], sems.at[1]),
            pltpu.make_async_copy(h_buf.at[half, c], hidden.at[:, at], sems.at[2]),
        )

    for half in range(2):
        @pl.loop(0, chunks)
        def _(c):
            for copy in copies(half, c):
                copy.start()

    for k, ref in enumerate((p_buf, m_buf, h_buf)):
        pltpu.make_async_copy(ref, ref, sems.at[k]).wait()


def solution(mesh):
    groups, shards = mesh.shape["rep"], mesh.shape["fsdp"]

    def body(tokens, norm_gain, outer_params, momentum, deltas):
        rows, model = tokens.shape
        _, height, hid = outer_params.shape
        chunks = hid // (2 * WIDTH)
        tall = height // 2
        bf16, f32 = jnp.bfloat16, jnp.float32
        dma = pltpu.SemaphoreType.DMA
        anywhere = pl.BlockSpec(memory_space=pl.ANY)
        inside = pl.BlockSpec(memory_space=pltpu.VMEM)
        quarters = (4, tall, hid)

        def strip(*lead):
            return pltpu.VMEM((chunks, *lead, tall, WIDTH), bf16)

        each, two = dma((chunks,)), dma((chunks, 2))
        p_next, m_next, h_next = pl.pallas_call(
            functools.partial(kernel, groups, shards),
            out_shape=(
                pltpu.VMEM((chunks, 4, 2, tall, WIDTH), f32),
                pltpu.VMEM((chunks, 4, 2, tall, WIDTH), f32),
                pltpu.VMEM((2, chunks, rows, WIDTH), bf16),
            ),
            in_specs=[anywhere, inside, anywhere, anywhere, anywhere],
            out_specs=(inside, inside, inside),
            scratch_shapes=[
                strip(2, 2, 4, 2, 2),
                strip(4, 2), strip(2, 2), strip(2), strip(2), strip(2), strip(2), strip(4, 2),
                pltpu.VMEM((2, rows, model), bf16),
                pltpu.VMEM((rows, model), bf16),
                pltpu.VMEM((chunks, rows, WIDTH), bf16),
                pltpu.VMEM((chunks, 2, 2, tall - ZROWS, WIDTH), bf16),
                pltpu.VMEM((chunks, ZROWS, WIDTH), bf16),
                each, two, dma,
                each, each, each, each, each, each, each, each, two, each, each, each,
                two, each, each, each, each, each, each, two, each, dma, dma,
                dma((2,)), dma((2,)), dma, dma((2,)), dma((2,)), dma, dma,
                dma, dma((2,)), dma((2,)), dma((2,)), dma((2,)),
                dma((2,)), dma((2,)), dma, dma, dma, dma((3,)), dma, dma((2,)), dma((2,)), dma, dma,
            ],
            compiler_params=pltpu.CompilerParams(
                collective_id=0, has_side_effects=True, vmem_limit_bytes=VMEM_LIMIT),
            name="round",
        )(
            tokens, norm_gain.reshape(1, model), outer_params.reshape(quarters), momentum.reshape(quarters),
            deltas.reshape(quarters),
        )
        new_params, new_momentum, hidden = pl.pallas_call(
            settle,
            out_shape=(
                jax.ShapeDtypeStruct(quarters, f32),
                jax.ShapeDtypeStruct(quarters, f32),
                jax.ShapeDtypeStruct((rows, hid), bf16),
            ),
            in_specs=[inside, inside, inside],
            out_specs=(anywhere, anywhere, anywhere),
            scratch_shapes=[dma((3,))],
            compiler_params=pltpu.CompilerParams(vmem_limit_bytes=4 * 1024 * 1024),
            name="settle",
        )(p_next, m_next, h_next)
        return (new_params.reshape(outer_params.shape), new_momentum.reshape(momentum.shape), hidden)

    in_specs = (
        P(("rep", "fsdp"), None),
        P(),
        P(None, "fsdp", None),
        P(None, "fsdp", None),
        P("rep", None, "fsdp", None),
    )
    out_specs = (P(None, "fsdp", None), P(None, "fsdp", None), P(("rep", "fsdp"), None))
    return jax.shard_map(body, mesh=mesh, in_specs=in_specs, out_specs=out_specs, check_vma=False)
```
